32 devices in a mesh: dp: 4 (over y, x), centers: 8 (over z, core).
Axes of the slice: x: 2, y: 2, z: 4, core: 2. Of those that a mesh axis runs over, the one named last changes fastest.
Arguments:
- points: bfloat16 [16384, 32], P('dp'), may hold values from -6 to 6
- centers: bfloat16 [16384, 32], P('centers'), may hold values from -6 to 6
- coef: bfloat16 [16384, 64], P('centers'), may hold values from -0.1875 to 0.1875
Outputs:
- product: float32 [16384, 64], P('centers')
The draws below stay inside these ranges and needn't reach their ends.
All inputs are finite; a program needn't handle non-finite values.
Results may differ from the reference program's by a relative error of at most 0.0003.
Values may be sent and summed in bfloat16 or wider, within the bound.
A program may use at most 128 MiB of HBM per device.

```python
import jax
import jax.numpy as jnp
from jax import lax

DIM = 32
OUTS = 64
NPTS = 16384
CENTERS = 16384


def block_scale(key, shape, shards, low, top_value):
    gain, own = 1.0, jax.random.fold_in(key, 6)
    for axis_at, blocks in shards:
        heights = jnp.exp(jax.random.uniform(jax.random.fold_in(own, axis_at), (blocks,), jnp.float32, low / len(shards), top_value / len(shards)))
        gain = gain * jnp.repeat(heights, shape[axis_at] // blocks).reshape([-1 if axis == axis_at else 1 for axis in range(len(shape))])
    return gain


def scatter_about(rng, shape, scale, limit, cuts=(), kind=jnp.bfloat16):
    values = jax.random.normal(rng, shape, jnp.float32) * scale
    if len(cuts) > 0:
        values = block_scale(rng, shape, cuts, -0.22, 0.18) * values
    return jnp.clip(values, min=-limit, max=limit).astype(kind)


def setup_inputs(seed: int = 0) -> dict:
    key_list = jax.random.split(jax.random.key(seed), 4)
    return {
        "points": scatter_about(key_list[0], (NPTS, DIM), 1.0, 6.0, ((0, 4),)),
        "centers": scatter_about(key_list[1], (CENTERS, DIM), 1.0, 6.0, ((0, 8),)),
        "coef": scatter_about(key_list[2], (CENTERS, OUTS), (CENTERS // 16) ** -0.5, 0.1875, ((0, 8),)),
    }


def kernel_block(left_pts, left_sq, right_pts, right_sq, features):
    inner = lax.dot_general(left_pts, right_pts, (((1,), (1,)), ((), ())), preferred_element_type=jnp.float32)
    dist = left_sq[:, None] + right_sq[None, :] - 2.0 * inner
    return jnp.exp(dist * (-2.0 / features)).astype(jnp.bfloat16)

def squares(values):
    wide = values.astype(jnp.float32)
    return lax.optimization_barrier(jnp.sum(wide * wide, axis=1))

def reference(points, centers, coef):
    features = points.shape[1]
    total_pts = points.shape[0]
    total_cen = centers.shape[0]
    outs_count = coef.shape[1]
    block_pts = min(1024, total_pts)
    cen_sq = squares(centers)
    point_blocks = points.reshape(total_pts // block_pts, block_pts, features)

    def data_step(accum, block):
        kernel = kernel_block(block, squares(block), centers, cen_sq, features)
        forward = jnp.dot(kernel, coef, preferred_element_type=jnp.float32).astype(jnp.bfloat16)
        back = lax.dot_general(kernel, forward, (((0,), (0,)), ((), ())), preferred_element_type=jnp.float32)
        return (accum + back, jnp.zeros((), jnp.float32))
    accum, unused = lax.scan(data_step, jnp.zeros((total_cen, outs_count), jnp.float32), point_blocks)
    block_cen = min(1024, total_cen)
    center_blocks = centers.reshape(total_cen // block_cen, block_cen, features)

    def center_step(carry, block):
        kernel = kernel_block(block, squares(block), centers, cen_sq, features)
        return (carry, jnp.dot(kernel, coef, preferred_element_type=jnp.float32))
    unused_two, regular = lax.scan(center_step, jnp.zeros((), jnp.float32), center_blocks)
    regular = regular.reshape(total_cen, outs_count)
    return accum * (1.0 / jnp.sqrt(jnp.float32(total_pts))) + regular
```

```python
import functools
import math

import jax
import jax.numpy as jnp
from jax import lax
from jax.experimental import pallas as pl
from jax.experimental.pallas import tpu as pltpu
from jax.sharding import PartitionSpec as P

MESH = pl.DeviceIdType.MESH
F32, BF16 = jnp.float32, jnp.bfloat16


def dot(a, b):
    return lax.dot_general(a, b, (((1,), (0,)), ((), ())), preferred_element_type=F32)


def dot_nt(a, b):
    return lax.dot_general(a, b, (((1,), (1,)), ((), ())), preferred_element_type=F32)


def split3(v):
    hi = v.astype(BF16).astype(F32)
    mid = (v - hi).astype(BF16).astype(F32)
    return hi, mid, (v - hi) - mid


def row_form(x, width):
    feats = x.shape[1]
    lane = lax.broadcasted_iota(jnp.int32, (feats, width), 1)
    sub = lax.broadcasted_iota(jnp.int32, (feats, width), 0)
    pick = ((lane % feats) == sub) & (lane < 3 * feats)
    spread = dot(x, pick.astype(F32).astype(BF16))
    wide = x.astype(F32)
    sq = jnp.sum(wide * wide, axis=1, keepdims=True) * (-2.0 * math.log2(math.e) / feats)
    hi, mid, lo = split3(sq)
    at = lax.broadcasted_iota(jnp.int32, (x.shape[0], width), 1) - 3 * feats
    tail = jnp.where(at == 3, hi, jnp.where(at == 4, mid, jnp.where(at == 5, lo, 0.0)))
    tail = jnp.where((at >= 0) & (at < 3), 1.0, tail)
    return (spread + tail).astype(BF16)


def col_form(ct, width):
    feats, count = ct.shape
    wide = ct.astype(F32)
    parts = [p.astype(BF16) for p in split3(wide * (4.0 * math.log2(math.e) / feats))]
    sq = jnp.sum(wide * wide, axis=0, keepdims=True) * (-2.0 * math.log2(math.e) / feats)
    hi, mid, lo = split3(sq)
    at = lax.broadcasted_iota(jnp.int32, (width - 3 * feats, count), 0)
    tail = jnp.where(at == 0, hi, jnp.where(at == 1, mid, jnp.where(at == 2, lo, 0.0)))
    tail = jnp.where((at >= 3) & (at < 6), 1.0, tail)
    return jnp.concatenate(parts + [tail.astype(BF16)], axis=0)


def kern(rows, cols):
    return jnp.exp2(dot(rows, cols)).astype(BF16)


def body(cfg, pts, cen, packed, out, kmat, colt, rowc, gath, reg, own_half, snd1, rcv1, snd2, rcv2,
         own_sum, fwd, csend, crecv, cown, full,
         as_, ar, fs, fr, b1s, b1r, b2s, b2r, gs, gr, hs, hr, cs, cr, ds_, dr):
    n_dp, n_c, feats, width = cfg
    n_h = n_c // 2
    d = lax.axis_index("dp")
    j = lax.axis_index("centers")
    par = lax.rem(j, 2)
    z = j // 2
    sib = j + 1 - 2 * par
    local_pts = pts.shape[0]
    local_cen = cen.shape[0]
    share = local_pts // n_c
    quarter = local_cen // n_dp
    step = min(512, local_cen)
    alpha_scale = 1.0 / math.sqrt(local_pts * n_dp)

    def up(t):
        return lax.rem(z + 1 + t, n_h)

    def down(t):
        return lax.rem(z + 2 * n_h - 1 - t, n_h)

    def dup(t):
        return lax.rem(d + 1 + t, n_dp)

    def ddown(t):
        return lax.rem(d + 2 * n_dp - 1 - t, n_dp)

    def copy(src, dst, ssem, rsem, dev):
        return pltpu.make_async_remote_copy(
            src_ref=src, dst_ref=dst, send_sem=ssem, recv_sem=rsem, device_id=dev, device_id_type=MESH
        )

    barrier = pltpu.get_barrier_semaphore()
    for t in range(n_h - 1):
        pl.semaphore_signal(barrier, inc=1, device_id=(d, 2 * up(t) + par), device_id_type=MESH)
    pl.semaphore_signal(barrier, inc=1, device_id=(d, sib), device_id_type=MESH)
    for t in range(n_dp - 1):
        pl.semaphore_signal(barrier, inc=1, device_id=(dup(t), j), device_id_type=MESH)

    for c in range(local_cen // step):
        at = pl.ds(c * step, step)
        colt[:, at] = col_form(packed[:feats, at], width)
        rowc[at, :] = row_form(cen[at, :], width)
    reg[...] = jnp.zeros_like(reg)

    pl.semaphore_wait(barrier, n_h - 1 + 1 + n_dp - 1)

    mine = packed.at[:, pl.ds(pl.multiple_of(d * quarter, 128), quarter)]

    def gather(t):
        return copy(mine, gath.at[j], as_.at[t], ar.at[t], (d, 2 * up(t) + par))

    def gather_in(t):
        return copy(mine, gath.at[2 * down(t) + par], as_.at[t], ar.at[t], (d, 2 * up(t) + par))

    for t in range(n_h - 1):
        gather(t).start()
    own_to_sib = copy(mine, gath.at[j], fs.at[n_h - 1], fr.at[n_h - 1], (d, sib))
    own_to_sib.start()
    gath[j] = packed[:, pl.ds(pl.multiple_of(d * quarter, 128), quarter)]

    def to_sib(t):
        return copy(snd1.at[t], rcv1.at[t], b1s.at[t], b1r.at[t], (d, sib))

    def to_peer(t):
        return copy(snd2.at[t], rcv2.at[t], b2s.at[t], b2r.at[t], (d, 2 * up(t) + par))

    def half(s):
        at = pl.ds(pl.multiple_of(s * share, share), share)
        rows = row_form(pts[at, :], width)
        acc = jnp.zeros((packed.shape[0] - feats, share), F32)
        for c in range(local_cen // step):
            cols = pl.ds(c * step, step)
            tile = kern(rows, colt[:, cols])
            kmat[at, cols] = tile
            acc = acc + dot_nt(packed[feats:, cols], tile)
        return acc

    @pl.loop(0, n_h)
    def _(t):
        zt = up(t)
        snd1[t] = half(2 * zt + 1 - par).astype(BF16)
        to_sib(t).start()
        own_half[...] = half(2 * zt + par)
        to_sib(t).wait_recv()
        total = own_half[...] + rcv1[t].astype(F32)

        @pl.when(t < n_h - 1)
        def _():
            snd2[t] = total.astype(BF16)
            to_peer(t).start()

        @pl.when(t == n_h - 1)
        def _():
            own_sum[...] = total

    def forward_block(t):
        at = gath.at[2 * down(t) + par]
        return copy(at, at, fs.at[t], fr.at[t], (d, sib))

    def forward_in(t):
        at = gath.at[2 * down(t) + 1 - par]
        return copy(at, at, fs.at[t], fr.at[t], (d, sib))

    for t in range(n_h - 1):
        gather_in(t).wait_recv()
        forward_block(t).start()

    def regular(block):
        cols = col_form(gath[block, :feats, :], width)
        weights = gath[block, feats:, :]
        for r in range(local_cen // step):
            rows = pl.ds(r * step, step)
            reg[:, rows] += dot_nt(weights, kern(rowc[rows, :], cols))

    @pl.loop(0, n_h)
    def _(i):
        regular(2 * i + par)

    for t in range(n_h - 1):
        to_peer(t).wait_recv()
    total = own_sum[...]
    for t in range(n_h - 1):
        total = total + rcv2[t].astype(F32)

    def slot(s):
        return fwd.at[:, pl.ds(pl.multiple_of(s * share, share), share)]

    def spread(t):
        return copy(slot(j), slot(j), gs.at[t], gr.at[t], (d, 2 * up(t) + par))

    def spread_in(t):
        at = slot(2 * down(t) + par)
        return copy(at, at, gs.at[t], gr.at[t], (d, 2 * up(t) + par))

    fwd[:, pl.ds(pl.multiple_of(j * share, share), share)] = total.astype(BF16)
    for t in range(n_h - 1):
        spread(t).start()
    own_fwd = copy(slot(j), slot(j), hs.at[n_h - 1], hr.at[n_h - 1], (d, sib))
    own_fwd.start()

    for t in range(n_h - 1):
        forward_in(t).wait_recv()
    own_sib_in = gath.at[sib]
    copy(own_sib_in, own_sib_in, fs.at[n_h - 1], fr.at[n_h - 1], (d, sib)).wait_recv()

    cut = (n_h * 3) // 4

    @pl.loop(0, cut)
    def _(i):
        regular(2 * i + 1 - par)

    def relay(t):
        at = slot(2 * down(t) + par)
        return copy(at, at, hs.at[t], hr.at[t], (d, sib))

    def relay_in(t):
        at = slot(2 * down(t) + 1 - par)
        return copy(at, at, hs.at[t], hr.at[t], (d, sib))

    for t in range(n_h - 1):
        spread_in(t).wait_recv()
        relay(t).start()

    @pl.loop(cut, n_h)
    def _(i):
        regular(2 * i + 1 - par)

    for t in range(n_h - 1):
        relay_in(t).wait_recv()
    copy(slot(sib), slot(sib), hs.at[n_h - 1], hr.at[n_h - 1], (d, sib)).wait_recv()

    def cross(t):
        return copy(csend.at[t], crecv.at[t], cs.at[t], cr.at[t], (dup(t), j))

    @pl.loop(0, n_dp)
    def _(t):
        at = pl.ds(pl.multiple_of(dup(t) * quarter, 128), quarter)
        back = dot(fwd[...], kmat[:, at]) * alpha_scale + reg[:, at]

        @pl.when(t < n_dp - 1)
        def _():
            csend[t] = back
            cross(t).start()

        @pl.when(t == n_dp - 1)
        def _():
            cown[...] = back

    for t in range(n_dp - 1):
        cross(t).wait_recv()
    total = cown[...]
    for t in range(n_dp - 1):
        total = total + crecv[t]
    full[d] = total

    def publish(t):
        return copy(full.at[d], full.at[d], ds_.at[t], dr.at[t], (dup(t), j))

    def publish_in(t):
        at = full.at[ddown(t)]
        return copy(at, at, ds_.at[t], dr.at[t], (dup(t), j))

    for t in range(n_dp - 1):
        publish(t).start()
    for t in range(n_h - 1):
        gather(t).wait_send()
        forward_block(t).wait_send()
        to_peer(t).wait_send()
        spread(t).wait_send()
        relay(t).wait_send()
    for t in range(n_h):
        to_sib(t).wait_send()
    own_to_sib.wait_send()
    own_fwd.wait_send()
    for t in range(n_dp - 1):
        cross(t).wait_send()
    for t in range(n_dp - 1):
        publish_in(t).wait_recv()
    for t in range(n_dp - 1):
        publish(t).wait_send()
    for q in range(n_dp):
        out[:, q * quarter:(q + 1) * quarter] = full[q]


def solution(mesh):
    n_dp, n_c = mesh.shape["dp"], mesh.shape["centers"]

    def on_device(points, centers, coef):
        local_pts, feats = points.shape
        local_cen, outs = coef.shape
        width = -(-(3 * feats + 6) // 128) * 128
        n_h = n_c // 2
        share, quarter = local_pts // n_c, local_cen // n_dp
        packed = jnp.concatenate([centers, coef], axis=1).T
        dma = pltpu.SemaphoreType.DMA
        result = pl.pallas_call(
            functools.partial(body, (n_dp, n_c, feats, width)),
            out_shape=jax.ShapeDtypeStruct((outs, local_cen), F32),
            in_specs=[pl.BlockSpec(memory_space=pltpu.VMEM)] * 3,
            out_specs=pl.BlockSpec(memory_space=pltpu.VMEM),
            scratch_shapes=[
                pltpu.VMEM((local_pts, local_cen), BF16),
                pltpu.VMEM((width, local_cen), BF16),
                pltpu.VMEM((local_cen, width), BF16),
                pltpu.VMEM((n_c, feats + outs, quarter), BF16),
                pltpu.VMEM((outs, local_cen), F32),
                pltpu.VMEM((outs, share), F32),
                pltpu.VMEM((n_h, outs, share), BF16),
                pltpu.VMEM((n_h, outs, share), BF16),
                pltpu.VMEM((n_h, outs, share), BF16),
                pltpu.VMEM((n_h, outs, share), BF16),
                pltpu.VMEM((outs, share), F32),
                pltpu.VMEM((outs, local_pts), BF16),
                pltpu.VMEM((n_dp, outs, quarter), F32),
                pltpu.VMEM((n_dp, outs, quarter), F32),
                pltpu.VMEM((outs, quarter), F32),
                pltpu.VMEM((n_dp, outs, quarter), F32),
            ] + [dma((n_h,))] * 12 + [dma((n_dp,))] * 4,
            compiler_params=pltpu.CompilerParams(
                collective_id=0, has_side_effects=True, vmem_limit_bytes=60 * 1024 * 1024
            ),
        )(points, centers, packed)
        return result.T

    return jax.shard_map(
        on_device,
        mesh=mesh,
        in_specs=(P("dp", None), P("centers", None), P("centers", None)),
        out_specs=P("centers", None),
        check_vma=False,
    )
```

```python
import functools
import math

import jax
import jax.numpy as jnp
from jax import lax
from jax.experimental import pallas as pl
from jax.experimental.pallas import tpu as pltpu
from jax.sharding import PartitionSpec as P

MESH = pl.DeviceIdType.MESH
F32, BF16 = jnp.float32, jnp.bfloat16


def dot(a, b):
    return lax.dot_general(a, b, (((1,), (0,)), ((), ())), preferred_element_type=F32)


def dot_nt(a, b):
    return lax.dot_general(a, b, (((1,), (1,)), ((), ())), preferred_element_type=F32)


def split3(v):
    hi = v.astype(BF16).astype(F32)
    mid = (v - hi).astype(BF16).astype(F32)
    return hi, mid, (v - hi) - mid


def row_form(x, width):
    feats = x.shape[1]
    lane = lax.broadcasted_iota(jnp.int32, (feats, width), 1)
    sub = lax.broadcasted_iota(jnp.int32, (feats, width), 0)
    pick = ((lane % feats) == sub) & (lane < 3 * feats)
    spread = dot(x, pick.astype(F32).astype(BF16))
    wide = x.astype(F32)
    sq = jnp.sum(wide * wide, axis=1, keepdims=True) * (-2.0 * math.log2(math.e) / feats)
    hi, mid, lo = split3(sq)
    at = lax.broadcasted_iota(jnp.int32, (x.shape[0], width), 1) - 3 * feats
    tail = jnp.where(at == 3, hi, jnp.where(at == 4, mid, jnp.where(at == 5, lo, 0.0)))
    tail = jnp.where((at >= 0) & (at < 3), 1.0, tail)
    return (spread + tail).astype(BF16)


def col_form(ct, width):
    feats, count = ct.shape
    wide = ct.astype(F32)
    parts = [p.astype(BF16) for p in split3(wide * (4.0 * math.log2(math.e) / feats))]
    sq = jnp.sum(wide * wide, axis=0, keepdims=True) * (-2.0 * math.log2(math.e) / feats)
    hi, mid, lo = split3(sq)
    at = lax.broadcasted_iota(jnp.int32, (width - 3 * feats, count), 0)
    tail = jnp.where(at == 0, hi, jnp.where(at == 1, mid, jnp.where(at == 2, lo, 0.0)))
    tail = jnp.where((at >= 3) & (at < 6), 1.0, tail)
    return jnp.concatenate(parts + [tail.astype(BF16)], axis=0)


def kern(rows, cols):
    return jnp.exp2(dot(rows, cols)).astype(BF16)


def body(cfg, pts_hbm, cen_hbm, packed, out, pts, cen, lsem, sibp, kmat, colt, rowc, gath, reg, own_half, snd1, rcv1, snd2, rcv2,
         own_sum, fwd, csend, crecv, cown, full,
         as_, ar, fs, fr, b1s, b1r, b2s, b2r, gs, gr, hs, hr, cs, cr, ds_, dr):
    n_dp, n_c, feats, width = cfg
    n_h = n_c // 2
    d = lax.axis_index("dp")
    j = lax.axis_index("centers")
    par = lax.rem(j, 2)
    z = j // 2
    sib = j + 1 - 2 * par
    local_pts = pts.shape[0]
    local_cen = cen.shape[0]
    share = local_pts // n_c
    quarter = local_cen // n_dp
    step = min(1024, local_cen)
    alpha_scale = 1.0 / math.sqrt(local_pts * n_dp)

    def up(t):
        return lax.rem(z + 1 + t, n_h)

    def down(t):
        return lax.rem(z + 2 * n_h - 1 - t, n_h)

    def dup(t):
        return lax.rem(d + 1 + t, n_dp)

    def ddown(t):
        return lax.rem(d + 2 * n_dp - 1 - t, n_dp)

    def copy(src, dst, ssem, rsem, dev):
        return pltpu.make_async_remote_copy(
            src_ref=src, dst_ref=dst, send_sem=ssem, recv_sem=rsem, device_id=dev, device_id_type=MESH
        )

    barrier = pltpu.get_barrier_semaphore()
    for t in range(n_h - 1):
        pl.semaphore_signal(barrier, inc=1, device_id=(d, 2 * up(t) + par), device_id_type=MESH)
    pl.semaphore_signal(barrier, inc=1, device_id=(d, sib), device_id_type=MESH)
    for t in range(n_dp - 1):
        pl.semaphore_signal(barrier, inc=1, device_id=(dup(t), j), device_id_type=MESH)

    cen_in = pltpu.make_async_copy(cen_hbm, cen, lsem.at[0])
    pts_in = pltpu.make_async_copy(pts_hbm, pts, lsem.at[1])
    cen_in.start()
    pts_in.start()
    for c in range(local_cen // step):
        at = pl.ds(c * step, step)
        colt[:, at] = col_form(packed[:feats, at], width)
    cen_in.wait()
    for c in range(local_cen // step):
        at = pl.ds(c * step, step)
        rowc[at, :] = row_form(cen[at, :], width)
    reg[...] = jnp.zeros_like(reg)

    pl.semaphore_wait(barrier, n_h - 1 + 1 + n_dp - 1)

    mine = packed.at[:, pl.ds(pl.multiple_of(d * quarter, 128), quarter)]

    def gather(t):
        return copy(mine, gath.at[j], as_.at[t], ar.at[t], (d, 2 * up(t) + par))

    def gather_in(t):
        return copy(mine, gath.at[2 * down(t) + par], as_.at[t], ar.at[t], (d, 2 * up(t) + par))

    for t in range(n_h - 1):
        gather(t).start()
    own_to_sib = copy(packed, sibp, fs.at[n_h - 1], fr.at[n_h - 1], (d, sib))
    own_to_sib.start()
    pts_in.wait()

    def to_sib(t):
        return copy(snd1.at[t], rcv1.at[t], b1s.at[t], b1r.at[t], (d, sib))

    def to_peer(t):
        return copy(snd2.at[t], rcv2.at[t], b2s.at[t], b2r.at[t], (d, 2 * up(t) + par))

    def half(s):
        at = pl.ds(pl.multiple_of(s * share, share), share)
        rows = row_form(pts[at, :], width)
        acc = jnp.zeros((packed.shape[0] - feats, share), F32)
        for c in range(local_cen // step):
            cols = pl.ds(c * step, step)
            tile = kern(rows, colt[:, cols])
            kmat[at, cols] = tile
            acc = acc + dot_nt(packed[feats:, cols], tile)
        return acc

    @pl.loop(0, n_h)
    def _(t):
        zt = up(t)
        snd1[t] = half(2 * zt + 1 - par).astype(BF16)
        to_sib(t).start()
        own_half[...] = half(2 * zt + par)
        to_sib(t).wait_recv()
        total = own_half[...] + rcv1[t].astype(F32)

        @pl.when(t < n_h - 1)
        def _():
            snd2[t] = total.astype(BF16)
            to_peer(t).start()

        @pl.when(t == n_h - 1)
        def _():
            own_sum[...] = total

    def forward_block(t):
        at = gath.at[2 * down(t) + par]
        return copy(at, at, fs.at[t], fr.at[t], (d, sib))

    def forward_in(t):
        at = gath.at[2 * down(t) + 1 - par]
        return copy(at, at, fs.at[t], fr.at[t], (d, sib))

    for t in range(n_h - 1):
        gather_in(t).wait_recv()
        forward_block(t).start()

    def regular(block):
        cols = col_form(gath[block, :feats, :], width)
        weights = gath[block, feats:, :]
        for r in range(local_cen // step):
            rows = pl.ds(r * step, step)
            reg[:, rows] += dot_nt(weights, kern(rowc[rows, :], cols))

    for t in range(n_h - 1):
        to_peer(t).wait_recv()
    total = own_sum[...]
    for t in range(n_h - 1):
        total = total + rcv2[t].astype(F32)

    def slot(s):
        return fwd.at[:, pl.ds(pl.multiple_of(s * share, share), share)]

    def spread(t):
        return copy(slot(j), slot(j), gs.at[t], gr.at[t], (d, 2 * up(t) + par))

    def spread_in(t):
        at = slot(2 * down(t) + par)
        return copy(at, at, gs.at[t], gr.at[t], (d, 2 * up(t) + par))

    fwd[:, pl.ds(pl.multiple_of(j * share, share), share)] = total.astype(BF16)
    for t in range(n_h - 1):
        spread(t).start()
    own_fwd = copy(slot(j), slot(j), hs.at[n_h - 1], hr.at[n_h - 1], (d, sib))
    own_fwd.start()

    @pl.loop(0, n_h - 1)
    def _(i):
        regular(2 * up(i) + par)

    for t in range(n_h - 1):
        forward_in(t).wait_recv()

    cut = ((n_h - 1) * 2) // 3

    @pl.loop(0, cut)
    def _(i):
        regular(2 * up(i) + 1 - par)

    def relay(t):
        at = slot(2 * down(t) + par)
        return copy(at, at, hs.at[t], hr.at[t], (d, sib))

    def relay_in(t):
        at = slot(2 * down(t) + 1 - par)
        return copy(at, at, hs.at[t], hr.at[t], (d, sib))

    for t in range(n_h - 1):
        spread_in(t).wait_recv()
        relay(t).start()

    @pl.loop(cut, n_h - 1)
    def _(i):
        regular(2 * up(i) + 1 - par)

    for t in range(n_h - 1):
        relay_in(t).wait_recv()
    copy(slot(sib), slot(sib), hs.at[n_h - 1], hr.at[n_h - 1], (d, sib)).wait_recv()

    def cross(t):
        return copy(csend.at[t], crecv.at[t], cs.at[t], cr.at[t], (dup(t), j))

    @pl.loop(0, n_dp)
    def _(t):
        at = pl.ds(pl.multiple_of(dup(t) * quarter, 128), quarter)
        back = dot(fwd[...], kmat[:, at]) * alpha_scale + reg[:, at]

        @pl.when(t < n_dp - 1)
        def _():
            csend[t] = back
            cross(t).start()

        @pl.when(t == n_dp - 1)
        def _():
            cown[...] = back

    own_to_sib.wait_recv()
    mine_rows = rowc[pl.ds(pl.multiple_of(d * quarter, 128), quarter), :]
    for c in range(local_cen // step):
        at = pl.ds(c * step, step)
        cown[...] += dot_nt(packed[feats:, at], kern(mine_rows, colt[:, at]))
        cown[...] += dot_nt(sibp[feats:, at], kern(mine_rows, col_form(sibp[:feats, at], width)))

    for t in range(n_dp - 1):
        cross(t).wait_recv()
    total = cown[...]
    for t in range(n_dp - 1):
        total = total + crecv[t]
    full[d] = total

    def publish(t):
        return copy(full.at[d], full.at[d], ds_.at[t], dr.at[t], (dup(t), j))

    def publish_in(t):
        at = full.at[ddown(t)]
        return copy(at, at, ds_.at[t], dr.at[t], (dup(t), j))

    for t in range(n_dp - 1):
        publish(t).start()
    for t in range(n_h - 1):
        gather(t).wait_send()
        forward_block(t).wait_send()
        to_peer(t).wait_send()
        spread(t).wait_send()
        relay(t).wait_send()
    for t in range(n_h):
        to_sib(t).wait_send()
    own_to_sib.wait_send()
    own_fwd.wait_send()
    for t in range(n_dp - 1):
        cross(t).wait_send()
    for t in range(n_dp - 1):
        publish_in(t).wait_recv()
    for t in range(n_dp - 1):
        publish(t).wait_send()
    for q in range(n_dp):
        out[:, q * quarter:(q + 1) * quarter] = full[q]


def solution(mesh):
    n_dp, n_c = mesh.shape["dp"], mesh.shape["centers"]

    def on_device(points, centers, coef):
        local_pts, feats = points.shape
        local_cen, outs = coef.shape
        width = -(-(3 * feats + 6) // 128) * 128
        n_h = n_c // 2
        share, quarter = local_pts // n_c, local_cen // n_dp
        packed = jnp.concatenate([centers, coef], axis=1).T
        dma = pltpu.SemaphoreType.DMA
        result = pl.pallas_call(
            functools.partial(body, (n_dp, n_c, feats, width)),
            out_shape=jax.ShapeDtypeStruct((outs, local_cen), F32),
            in_specs=[pl.BlockSpec(memory_space=pl.ANY)] * 2 + [pl.BlockSpec(memory_space=pltpu.VMEM)],
            out_specs=pl.BlockSpec(memory_space=pltpu.VMEM),
            scratch_shapes=[
                pltpu.VMEM((local_pts, feats), BF16),
                pltpu.VMEM((local_cen, feats), BF16),
                dma((2,)),
                pltpu.VMEM((feats + outs, local_cen), BF16),
                pltpu.VMEM((local_pts, local_cen), BF16),
                pltpu.VMEM((width, local_cen), BF16),
                pltpu.VMEM((local_cen, width), BF16),
                pltpu.VMEM((n_c, feats + outs, quarter), BF16),
                pltpu.VMEM((outs, local_cen), F32),
                pltpu.VMEM((outs, share), F32),
                pltpu.VMEM((n_h, outs, share), BF16),
                pltpu.VMEM((n_h, outs, share), BF16),
                pltpu.VMEM((n_h, outs, share), BF16),
                pltpu.VMEM((n_h, outs, share), BF16),
                pltpu.VMEM((outs, share), F32),
                pltpu.VMEM((outs, local_pts), BF16),
                pltpu.VMEM((n_dp, outs, quarter), F32),
                pltpu.VMEM((n_dp, outs, quarter), F32),
                pltpu.VMEM((outs, quarter), F32),
                pltpu.VMEM((n_dp, outs, quarter), F32),
            ] + [dma((n_h,))] * 12 + [dma((n_dp,))] * 4,
            compiler_params=pltpu.CompilerParams(
                collective_id=0, has_side_effects=True, vmem_limit_bytes=60 * 1024 * 1024
            ),
        )(points, centers, packed)
        return result.T

    return jax.shard_map(
        on_device,
        mesh=mesh,
        in_specs=(P("dp", None), P("centers", None), P("centers", None)),
        out_specs=P("centers", None),
        check_vma=False,
    )
```
